32 devices in a mesh: dp: 1 (over z), tp: 4 (over y), ep: 8 (over x, core).
Axes of the slice: x: 4, y: 4, z: 1, core: 2. Of those that a mesh axis runs over, the one named last changes fastest.
The devices are a block of a 4x4x8 slice.
Arguments:
- x: bfloat16 [64, 1024, 768], P(('dp', 'ep'))
- src_len: int32 [64], P(('dp', 'ep'))
- expert_idx: int32 [64, 1024, 2], P(('dp', 'ep'))
- ln_gain: float32 [4, 768], replicated
- ln_bias: float32 [4, 768], replicated
- w_query: bfloat16 [2, 768, 12, 64], P(None, None, 'tp')
- b_query: float32 [2, 12, 64], P(None, 'tp')
- w_key: bfloat16 [2, 768, 12, 64], P(None, None, 'tp')
- w_value: bfloat16 [2, 768, 12, 64], P(None, None, 'tp')
- b_value: float32 [2, 12, 64], P(None, 'tp')
- w_attn_out: bfloat16 [2, 12, 64, 768], P(None, 'tp')
- b_attn_out: float32 [2, 768], replicated
- w_fc1: bfloat16 [768, 3072], P(None, 'tp')
- b_fc1: float32 [3072], P('tp')
- w_fc2: bfloat16 [3072, 768], P('tp')
- b_fc2: float32 [768], replicated
- w_router: float32 [768, 32], replicated
- w_exp_in: bfloat16 [32, 768, 3072], P('ep', None, 'tp')
- b_exp_in: float32 [32, 3072], P('ep', 'tp')
- w_exp_out: bfloat16 [32, 3072, 768], P('ep', 'tp')
- b_exp_out: float32 [32, 768], P('ep')
Outputs:
- output: bfloat16 [64, 1024, 768], P(('dp', 'ep'))
All inputs are finite; a program needn't handle non-finite values.
Results may differ from the reference program's by a relative error of at most 0.0144854.
Values are sent between devices in bfloat16 or wider.
A program may use at most 768 MiB of HBM per device.

```python
import jax
import jax.numpy as jnp
from jax import lax

GROUPS = 8
ROWS_DEV = 8
SEQ_LEN = 1024
D_MODEL = 768
NUM_HEADS = 12
HEAD_DIM = 64
FF_DENSE = 3072
EXPERTS = 32
EXPERT_FF = 3072

BATCH = GROUPS * ROWS_DEV
TOKENS_GROUP = ROWS_DEV * SEQ_LEN
CAPACITY = 2 * ((TOKENS_GROUP + EXPERTS - 1) // EXPERTS)
DUMP_SLOT = EXPERTS * CAPACITY
INNER_DIM = NUM_HEADS * HEAD_DIM
LN_EPS = 1e-5


def layer_norm(hidden, gain, shift):
    hidden = hidden.astype(jnp.float32)
    centered = hidden - jnp.mean(hidden, axis=-1, keepdims=True)
    variance = jnp.mean(centered * centered, axis=-1, keepdims=True)
    return centered * lax.rsqrt(variance + LN_EPS) * gain + shift


def draw_routing(route_key):
    len_key, hot_key, pick_key, first_key, second_key = jax.random.split(route_key, 5)
    row_ids = jnp.arange(BATCH)
    lengths = jax.random.randint(len_key, (BATCH,), SEQ_LEN // 4, SEQ_LEN + 1)
    lengths = jnp.where(row_ids == 0, SEQ_LEN, lengths)
    lengths = jnp.where(row_ids == BATCH - 1, SEQ_LEN // 4, lengths)
    hot_count = max(EXPERTS // 16, 1)
    hot_start = jax.random.randint(hot_key, (), 0, EXPERTS)
    grid = (BATCH, SEQ_LEN)
    pick_hot = jax.random.randint(pick_key, grid, 0, 4) == 0
    uniform_first = jax.random.randint(first_key, grid, 0, EXPERTS)
    hot_first = (hot_start + uniform_first % hot_count) % EXPERTS
    first = jnp.where(pick_hot, hot_first, uniform_first)
    second = (first + jax.random.randint(second_key, grid, 1, EXPERTS)) % EXPERTS
    expert_idx = jnp.stack([first, second], axis=-1).astype(jnp.int32)
    return lengths.astype(jnp.int32), expert_idx


def scaled_normal(key, extent, scale):
    return jax.random.normal(key, extent, jnp.float32) * scale


def setup_inputs(seed: int = 0, part: int = 0) -> dict:
    part_key = jax.random.fold_in(jax.random.key(seed), part)
    x_key, route_key = jax.random.split(part_key, 2)
    keys = jax.random.split(jax.random.key(seed + 1), 18)
    src_len, expert_idx = draw_routing(route_key)
    attn_shape = (2, D_MODEL, NUM_HEADS, HEAD_DIM)
    model_scale = D_MODEL ** -0.5
    inner_scale = INNER_DIM ** -0.5
    return {
        'x': scaled_normal(x_key, (BATCH, SEQ_LEN, D_MODEL), 1.0).astype(jnp.bfloat16),
        'src_len': src_len,
        'expert_idx': expert_idx,
        'ln_gain': 1.0 + scaled_normal(keys[0], (4, D_MODEL), 0.2),
        'ln_bias': scaled_normal(keys[1], (4, D_MODEL), 0.2),
        'w_query': scaled_normal(keys[2], attn_shape, model_scale).astype(jnp.bfloat16),
        'b_query': scaled_normal(keys[3], (2, NUM_HEADS, HEAD_DIM), 0.5),
        'w_key': scaled_normal(keys[4], attn_shape, model_scale).astype(jnp.bfloat16),
        'w_value': scaled_normal(keys[5], attn_shape, model_scale).astype(jnp.bfloat16),
        'b_value': scaled_normal(keys[6], (2, NUM_HEADS, HEAD_DIM), 0.5),
        'w_attn_out': scaled_normal(keys[7], (2, NUM_HEADS, HEAD_DIM, D_MODEL), inner_scale).astype(jnp.bfloat16),
        'b_attn_out': scaled_normal(keys[8], (2, D_MODEL), 0.3),
        'w_fc1': scaled_normal(keys[9], (D_MODEL, FF_DENSE), model_scale).astype(jnp.bfloat16),
        'b_fc1': scaled_normal(keys[10], (FF_DENSE,), 0.5),
        'w_fc2': scaled_normal(keys[11], (FF_DENSE, D_MODEL), FF_DENSE ** -0.5).astype(jnp.bfloat16),
        'b_fc2': scaled_normal(keys[12], (D_MODEL,), 0.3),
        'w_router': scaled_normal(keys[13], (D_MODEL, EXPERTS), model_scale),
        'w_exp_in': scaled_normal(keys[14], (EXPERTS, D_MODEL, EXPERT_FF), model_scale).astype(jnp.bfloat16),
        'b_exp_in': scaled_normal(keys[15], (EXPERTS, EXPERT_FF), 0.5),
        'w_exp_out': scaled_normal(keys[16], (EXPERTS, EXPERT_FF, D_MODEL), EXPERT_FF ** -0.5).astype(jnp.bfloat16),
        'b_exp_out': scaled_normal(keys[17], (EXPERTS, D_MODEL), 0.5),
    }


def attention_row(residual, key_ok, gain, shift, w_q, b_q, w_k, w_v, b_v, w_o, b_o):
    normed = layer_norm(residual, gain, shift).astype(jnp.bfloat16)

    def project(weight):
        flat = jnp.dot(normed, weight.reshape(D_MODEL, INNER_DIM), preferred_element_type=jnp.float32)
        return flat.reshape(SEQ_LEN, NUM_HEADS, HEAD_DIM)

    query = (project(w_q) + b_q).astype(jnp.bfloat16)
    keys = project(w_k).astype(jnp.bfloat16)
    values = (project(w_v) + b_v).astype(jnp.bfloat16)
    scores = jnp.einsum('qhk,shk->hqs', query.astype(jnp.float32), keys.astype(jnp.float32)) * (HEAD_DIM ** -0.5)
    scores = jnp.where(key_ok[None, None, :], scores, -1e30)
    attn_probs = jax.nn.softmax(scores, axis=-1).astype(jnp.bfloat16)
    context = jnp.einsum('hqs,shk->qhk', attn_probs.astype(jnp.float32), values.astype(jnp.float32)).astype(jnp.bfloat16)
    projected = jnp.dot(context.reshape(SEQ_LEN, INNER_DIM), w_o.reshape(INNER_DIM, D_MODEL), preferred_element_type=jnp.float32)
    return (residual.astype(jnp.float32) + projected + b_o).astype(jnp.bfloat16)


def dense_ffn(residual, gain, shift, w_in, b_in, w_out, b_out):
    normed = layer_norm(residual, gain, shift).astype(jnp.bfloat16)
    inner = jax.nn.relu(jnp.dot(normed, w_in, preferred_element_type=jnp.float32) + b_in).astype(jnp.bfloat16)
    projected = jnp.dot(inner, w_out, preferred_element_type=jnp.float32)
    return (residual.astype(jnp.float32) + projected + b_out).astype(jnp.bfloat16)


def take_rows(rows, index):
    return rows[index]


def fill_table(dest_first, dest_second):
    token_ids = jnp.arange(TOKENS_GROUP, dtype=jnp.int32)
    table = jnp.full((DUMP_SLOT + 1,), TOKENS_GROUP, jnp.int32)
    table = table.at[dest_first].set(token_ids).at[dest_second].set(token_ids)
    return table[:DUMP_SLOT]


def run_expert(operands):
    rows_in, w_in, b_in, w_out, b_out = operands
    inner = jax.nn.relu(jnp.dot(rows_in, w_in, preferred_element_type=jnp.float32) + b_in).astype(jnp.bfloat16)
    return (jnp.dot(inner, w_out, preferred_element_type=jnp.float32) + b_out).astype(jnp.bfloat16)


def reference(x, src_len, expert_idx, ln_gain, ln_bias, w_query, b_query, w_key, w_value, b_value, w_attn_out, b_attn_out, w_fc1, b_fc1, w_fc2, b_fc2, w_router, w_exp_in, b_exp_in, w_exp_out, b_exp_out):
    positions = jnp.arange(SEQ_LEN)

    def row_layers(row_pair):
        row, length = row_pair
        key_ok = positions < length
        hidden = attention_row(row, key_ok, ln_gain[0], ln_bias[0], w_query[0], b_query[0], w_key[0], w_value[0], b_value[0], w_attn_out[0], b_attn_out[0])
        hidden = dense_ffn(hidden, ln_gain[1], ln_bias[1], w_fc1, b_fc1, w_fc2, b_fc2)
        hidden = attention_row(hidden, key_ok, ln_gain[2], ln_bias[2], w_query[1], b_query[1], w_key[1], w_value[1], b_value[1], w_attn_out[1], b_attn_out[1])
        normed = layer_norm(hidden, ln_gain[3], ln_bias[3])
        logits = jnp.dot(normed, w_router, preferred_element_type=jnp.float32)
        return hidden, normed.astype(jnp.bfloat16), logits

    residual, normed, logits = lax.map(row_layers, (x, src_len))
    grouped = (GROUPS, TOKENS_GROUP)
    valid = (positions[None, :] < src_len[:, None]).reshape(grouped)
    first = expert_idx[..., 0].reshape(grouped)
    second = expert_idx[..., 1].reshape(grouped)
    router_probs = jax.nn.softmax(logits, axis=-1).reshape(GROUPS, TOKENS_GROUP, EXPERTS)
    prob_first = jnp.take_along_axis(router_probs, first[..., None], axis=-1)[..., 0]
    prob_second = jnp.take_along_axis(router_probs, second[..., None], axis=-1)[..., 0]
    gate_first = prob_first / (prob_first + prob_second)
    gate_second = prob_second / (prob_first + prob_second)
    expert_ids = jnp.arange(EXPERTS)
    hot_first = ((first[..., None] == expert_ids) & valid[..., None]).astype(jnp.int32)
    hot_second = ((second[..., None] == expert_ids) & valid[..., None]).astype(jnp.int32)
    rank_first = jnp.cumsum(hot_first, axis=1) - 1
    rank_second = jnp.cumsum(hot_second, axis=1) - 1 + jnp.sum(hot_first, axis=1, keepdims=True)
    slot_first = jnp.sum(rank_first * hot_first, axis=-1)
    slot_second = jnp.sum(rank_second * hot_second, axis=-1)
    dest_first = jnp.where(valid & (slot_first < CAPACITY), first * CAPACITY + slot_first, DUMP_SLOT)
    dest_second = jnp.where(valid & (slot_second < CAPACITY), second * CAPACITY + slot_second, DUMP_SLOT)
    tables = jax.vmap(fill_table)(dest_first, dest_second)
    zero_row = jnp.zeros((GROUPS, 1, D_MODEL), jnp.bfloat16)
    padded = jnp.concatenate([normed.reshape(GROUPS, TOKENS_GROUP, D_MODEL), zero_row], axis=1)
    dispatched = jax.vmap(take_rows)(padded, tables)
    per_expert = dispatched.reshape(GROUPS, EXPERTS, CAPACITY, D_MODEL).transpose(1, 0, 2, 3).reshape(EXPERTS, GROUPS * CAPACITY, D_MODEL)
    expert_out = lax.map(run_expert, (per_expert, w_exp_in, b_exp_in, w_exp_out, b_exp_out))
    returned = expert_out.reshape(EXPERTS, GROUPS, CAPACITY, D_MODEL).transpose(1, 0, 2, 3).reshape(GROUPS, DUMP_SLOT, D_MODEL)
    returned = jnp.concatenate([returned, zero_row], axis=1)
    out_first = jax.vmap(take_rows)(returned, dest_first).astype(jnp.float32)
    out_second = jax.vmap(take_rows)(returned, dest_second).astype(jnp.float32)
    combined = gate_first[..., None] * out_first + gate_second[..., None] * out_second
    result = residual.reshape(GROUPS, TOKENS_GROUP, D_MODEL).astype(jnp.float32) + combined
    return result.astype(jnp.bfloat16).reshape(BATCH, SEQ_LEN, D_MODEL)
```

```python
import functools

import jax
import jax.numpy as jnp
from jax import lax
from jax.experimental import pallas as pl
from jax.experimental.pallas import tpu as pltpu
from jax.sharding import PartitionSpec as P

LN_EPS = 1e-5
LOG2_E = 1.4426950408889634
UNROLL = 4


def layer_norm(hidden, gain, shift):
    hidden = hidden.astype(jnp.float32)
    centered = hidden - jnp.mean(hidden, axis=-1, keepdims=True)
    variance = jnp.mean(centered * centered, axis=-1, keepdims=True)
    return centered * lax.rsqrt(variance + LN_EPS) * gain + shift


def dot_rows(lhs, rhs):
    return lax.dot_general(lhs, rhs, (((1,), (0,)), ((), ())), preferred_element_type=jnp.float32)


def dot_cols(lhs, rhs):
    return lax.dot_general(lhs, rhs, (((1,), (1,)), ((), ())), preferred_element_type=jnp.float32)


def attention_kernel(head_dim, q_block, len_ref, q_ref, k_ref, v_ref, o_ref):
    seq, lanes = k_ref.shape
    real_keys = len_ref[pl.program_id(0)]
    scale = head_dim ** -0.5 * LOG2_E
    lane = lax.broadcasted_iota(jnp.int32, (1, lanes), 1)
    key_lane = lax.broadcasted_iota(jnp.int32, (seq, lanes), 1)
    key_ok = lax.broadcasted_iota(jnp.int32, (seq, lanes), 0) < real_keys
    pad_bias = jnp.where(key_ok, 0.0, -1e30)
    keys_f32 = k_ref[...].astype(jnp.float32)
    values = v_ref[...]
    heads = []
    for head in range(lanes // head_dim):
        spare = (head + 1) * head_dim % lanes
        own = (key_lane // head_dim == head) & key_ok
        heads.append((jnp.where(own, keys_f32, jnp.where(key_lane == spare, pad_bias, 0.0)).astype(jnp.bfloat16), spare))

    def block(i, carry):
        rows = pl.ds(pl.multiple_of(i * q_block, q_block), q_block)
        q_all = q_ref[rows, :].astype(jnp.float32)
        result = jnp.zeros((q_block, lanes), jnp.float32)
        for head, (keys, spare) in enumerate(heads):
            own = lane // head_dim == head
            query = jnp.where(own, q_all, jnp.where(lane == spare, 1.0, 0.0)).astype(jnp.bfloat16)
            scores = dot_cols(query, keys)
            top = jnp.max(scores, axis=-1, keepdims=True)
            weights = jnp.exp2((scores - top) * scale)
            total = jnp.sum(weights, axis=-1, keepdims=True)
            probs = (weights * (1.0 / total)).astype(jnp.bfloat16)
            result = jnp.where(own, dot_rows(probs, values), result)
        o_ref[rows, :] = result.astype(jnp.bfloat16)
        return carry

    lax.fori_loop(0, seq // q_block, block, 0, unroll=UNROLL)


def attend(query, keys, values, src_len, seq, head_dim):
    tokens, width = query.shape
    rows = tokens // seq
    lanes = 128
    spec = pl.BlockSpec((seq, lanes), lambda r, c, lens: (r, c))
    heads = width // head_dim
    return pl.pallas_call(
        functools.partial(attention_kernel, head_dim, 256),
        out_shape=jax.ShapeDtypeStruct((tokens, width), jnp.bfloat16),
        grid_spec=pltpu.PrefetchScalarGridSpec(num_scalar_prefetch=1, grid=(rows, width // lanes), in_specs=[spec, spec, spec], out_specs=spec),
        compiler_params=pltpu.CompilerParams(dimension_semantics=('arbitrary', 'arbitrary')),
        cost_estimate=pl.CostEstimate(flops=40 * rows * heads * seq * seq * head_dim, bytes_accessed=8 * tokens * width, transcendentals=rows * heads * seq * seq),
        name='attend',
    )(src_len, query, keys, values)


def attention_layer(residual, normed, src_len, seq, head_dim, w_q, b_q, w_k, w_v, b_v, w_o, b_o):
    query = (dot_cols(normed, w_q) + b_q).astype(jnp.bfloat16)
    keys = dot_cols(normed, w_k).astype(jnp.bfloat16)
    values = (dot_cols(normed, w_v) + b_v).astype(jnp.bfloat16)
    context = attend(query, keys, values, src_len, seq, head_dim)
    return (residual.astype(jnp.float32) + dot_rows(context, w_o) + b_o).astype(jnp.bfloat16)


def dense_ffn(residual, gain, shift, blocks, b_out):
    normed = layer_norm(residual, gain, shift).astype(jnp.bfloat16)
    projected = 0.0
    for w_in, b_in, w_out in blocks:
        inner = jax.nn.relu(dot_cols(normed, w_in) + b_in).astype(jnp.bfloat16)
        projected = projected + dot_rows(inner, w_out)
    return (residual.astype(jnp.float32) + projected + b_out).astype(jnp.bfloat16)


def route_slots(valid, first, second, num_experts, capacity):
    expert_ids = jnp.arange(num_experts, dtype=jnp.int32)
    hot_first = ((first[:, None] == expert_ids) & valid[:, None]).astype(jnp.int32)
    hot_second = ((second[:, None] == expert_ids) & valid[:, None]).astype(jnp.int32)
    rank_first = jnp.cumsum(hot_first, axis=0) - 1
    rank_second = jnp.cumsum(hot_second, axis=0) - 1 + jnp.sum(hot_first, axis=0)
    slot_first = jnp.sum(rank_first * hot_first, axis=1)
    slot_second = jnp.sum(rank_second * hot_second, axis=1)
    return slot_first, slot_second, valid & (slot_first < capacity), valid & (slot_second < capacity)


def solution(mesh):
    ep_size = mesh.shape['ep']
    tp_size = mesh.shape['tp']

    def gathered(shard):
        return lax.all_gather(shard, 'tp', axis=0, tiled=True)

    def local_fn(x, src_len, expert_idx, ln_gain, ln_bias, w_query, b_query, w_key, w_value, b_value, w_attn_out, b_attn_out, w_fc1, b_fc1, w_fc2, b_fc2, w_router, w_exp_in, b_exp_in, w_exp_out, b_exp_out):
        rows, seq_len, d_model = x.shape
        tokens = rows * seq_len
        num_experts = w_router.shape[1]
        capacity = 2 * (-(-tokens // num_experts))
        local_experts = w_exp_in.shape[0]
        layers, _, local_heads, head_dim = w_query.shape
        head_width = local_heads * head_dim
        part = capacity // tp_size
        own_rows = rows // tp_size
        me = lax.axis_index('tp')

        def whole(parts, height):
            return lax.all_gather(jnp.concatenate([w.reshape(-1, height, d_model) for w in parts], axis=0), 'tp', axis=1, tiled=True)

        def cols(w):
            return w.reshape(d_model, head_width).T

        biases = jnp.concatenate([b_query.reshape(-1), b_value.reshape(-1), b_fc1, b_exp_in.reshape(-1)])
        biases = lax.all_gather(biases, 'tp', axis=0)
        sizes = [layers * head_width, layers * head_width, b_fc1.shape[0], b_exp_in.size]
        offsets = [sum(sizes[:i]) for i in range(5)]
        b_q, b_v, b_in, b_expert = [biases[:, offsets[i]:offsets[i + 1]] for i in range(4)]
        b_q = b_q.reshape(tp_size, layers, head_width).transpose(1, 0, 2).reshape(layers, -1)
        b_v = b_v.reshape(tp_size, layers, head_width).transpose(1, 0, 2).reshape(layers, -1)
        b_expert = b_expert.reshape(tp_size, local_experts, -1).transpose(1, 0, 2).reshape(local_experts, -1)

        ep_me = lax.axis_index('ep')
        slab = w_fc1.shape[1] // ep_size
        slab_in = lax.dynamic_slice_in_dim(w_fc1, ep_me * slab, slab, 1).T
        slab_out = lax.dynamic_slice_in_dim(w_fc2, ep_me * slab, slab, 0)
        mine, choices = lax.optimization_barrier((whole([slab_in, slab_out], slab), expert_idx))
        cores = 2
        parts, owners = [mine], [ep_me]
        for step in range(cores, ep_size, cores):
            parts.append(lax.ppermute(mine, 'ep', [(e, (e + step) % ep_size) for e in range(ep_size)]))
            owners.append((ep_me + ep_size - step) % ep_size)
        core_half = jnp.concatenate(parts, axis=1)
        other_half = lax.ppermute(core_half, 'ep', [(e, e ^ 1) for e in range(ep_size)])
        owners = jnp.stack(owners)
        b_slabs = b_in.reshape(tp_size, ep_size, slab).transpose(1, 0, 2)

        def slab_bias(e):
            return jnp.sum(jnp.where((e[:, None] == jnp.arange(ep_size))[:, :, None, None], b_slabs[None], 0.0), axis=1).reshape(-1)

        sibling = ep_me + 1 - 2 * (ep_me % cores)
        other_owners = jnp.stack([(sibling + ep_size - step) % ep_size for step in range(0, ep_size, cores)])

        qkvo = whole([cols(w_query[0]), cols(w_key[0]), cols(w_value[0]), w_attn_out[0]], head_width)
        later = whole([cols(w_query[1]), cols(w_key[1]), cols(w_value[1]), w_attn_out[1]], head_width)
        second_weights = later[0], later[1], later[2], later[3]
        ff_part = w_exp_in.shape[2]

        def expert_weights(experts, after):
            parts, after = lax.optimization_barrier(([w for e in experts for w in (w_exp_in[e].T, w_exp_out[e])], after))
            both = whole(parts, ff_part)
            return [(both[2 * i], both[2 * i + 1]) for i in range(len(experts))], after


        dense_blocks = [(core_half[0], slab_bias(owners), core_half[1]), (other_half[0], slab_bias(other_owners), other_half[1])]
        first_weights = qkvo[0], qkvo[1], qkvo[2], qkvo[3]

        own_x = lax.dynamic_index_in_dim(x.reshape(own_rows, tp_size, seq_len, d_model), me, 1, keepdims=False).reshape(own_rows * seq_len, d_model)
        own_len = lax.dynamic_index_in_dim(src_len.reshape(own_rows, tp_size), me, 1, keepdims=False)

        def norm(v, i):
            return layer_norm(v, ln_gain[i], ln_bias[i]).astype(jnp.bfloat16)

        def attention(v, normed, lens, j, weights):
            w_q, w_k, w_v, w_o = weights
            return attention_layer(v, normed, lens, seq_len, head_dim, w_q, b_q[j], w_k, w_v, b_v[j], w_o, b_attn_out[j])

        expert_w, own_normed = expert_weights(list(range(local_experts // 2)), norm(own_x, 0))
        key_ok = jnp.arange(seq_len)[None, :] < src_len[:, None]
        valid = key_ok.reshape(tokens)
        first = choices[..., 0].reshape(tokens)
        second = choices[..., 1].reshape(tokens)
        slot_first, slot_second, keep_first, keep_second = route_slots(valid, first, second, num_experts, capacity)
        dump_slot = num_experts * capacity
        token_ids = jnp.arange(tokens, dtype=jnp.int32)
        table = jnp.zeros((dump_slot + 1,), jnp.int32)
        own_normed, slot_first, slot_second = lax.optimization_barrier((own_normed, slot_first, slot_second))
        own = attention(own_x, own_normed, own_len, 0, first_weights)
        own = dense_ffn(own, ln_gain[1], ln_bias[1], dense_blocks, b_fc2)
        chunks = []
        for c in range(own_rows):
            row = own[c * seq_len:(c + 1) * seq_len]
            out = attention(row, norm(row, 2), own_len[c:c + 1], 1, second_weights)
            if c == 0:
                out, expert_w[0] = lax.optimization_barrier((out, expert_w[0]))
            if c == own_rows - 1:
                more, out = expert_weights(list(range(local_experts // 2, local_experts)), out)
                expert_w += more
            chunks.append(gathered(out))

        table = table.at[jnp.where(keep_first, first * capacity + slot_first, dump_slot)].set(token_ids)
        table = table.at[jnp.where(keep_second, second * capacity + slot_second, dump_slot)].set(token_ids)
        table = table[:dump_slot].reshape(ep_size, local_experts, tp_size, part)
        table = lax.dynamic_index_in_dim(table, me, 2, keepdims=False)

        hidden = jnp.concatenate(chunks, axis=0)
        normed_f32 = layer_norm(hidden, ln_gain[3], ln_bias[3])
        logits = jnp.dot(normed_f32, w_router, preferred_element_type=jnp.float32)
        expert_ids = jnp.arange(num_experts, dtype=jnp.int32)
        logit_first = jnp.sum(jnp.where(first[:, None] == expert_ids, logits, 0.0), axis=1)
        logit_second = jnp.sum(jnp.where(second[:, None] == expert_ids, logits, 0.0), axis=1)
        gate_first = jax.nn.sigmoid(logit_first - logit_second)
        gate_second = jax.nn.sigmoid(logit_second - logit_first)

        normed = normed_f32.astype(jnp.bfloat16)
        returned = []
        pair = local_experts // 2
        starts = range(0, local_experts, pair)
        dispatch = [normed[table[:, start:start + pair].reshape(-1)].reshape(ep_size, pair, part, d_model) for start in starts]
        for n, start in enumerate(starts):
            received = lax.all_to_all(dispatch[n], 'ep', 0, 0, tiled=True)
            if n == 0:
                received, *dispatch[1:] = lax.optimization_barrier((received, *dispatch[1:]))
            outs = []
            for e in range(start, start + pair):
                w_in, w_out = expert_w[e]
                inner = jax.nn.relu(dot_cols(received[:, e - start].reshape(-1, d_model), w_in) + b_expert[e]).astype(jnp.bfloat16)
                outs.append((dot_rows(inner, w_out) + b_exp_out[e]).astype(jnp.bfloat16).reshape(ep_size, part, d_model))
            back = lax.all_to_all(jnp.stack(outs, axis=1), 'ep', 0, 0, tiled=True)
            returned.append(gathered(back.reshape(-1, d_model)))
        flat = jnp.concatenate(returned, axis=0)

        def place(expert, slot):
            owner, e = expert // local_experts, expert % local_experts
            return (((e // pair * tp_size + slot // part) * ep_size + owner) * pair + e % pair) * part + slot % part

        out_first = flat[jnp.where(keep_first, place(first, slot_first), 0)].astype(jnp.float32)
        out_second = flat[jnp.where(keep_second, place(second, slot_second), 0)].astype(jnp.float32)
        combined = jnp.where(keep_first[:, None], gate_first[:, None] * out_first, 0.0) + jnp.where(keep_second[:, None], gate_second[:, None] * out_second, 0.0)
        return (hidden.astype(jnp.float32) + combined).astype(jnp.bfloat16).reshape(rows, seq_len, d_model)

    in_specs = (P(('dp', 'ep'), None, None), P(('dp', 'ep')), P(('dp', 'ep'), None, None), P(), P(), P(None, None, 'tp', None), P(None, 'tp', None), P(None, None, 'tp', None), P(None, None, 'tp', None), P(None, 'tp', None), P(None, 'tp', None, None), P(), P(None, 'tp'), P('tp'), P('tp', None), P(), P(), P('ep', None, 'tp'), P('ep', 'tp'), P('ep', 'tp', None), P('ep', None))
    return jax.shard_map(local_fn, mesh=mesh, in_specs=in_specs, out_specs=P(('dp', 'ep'), None, None), check_vma=False)
```

```python
import functools

import jax
import jax.numpy as jnp
from jax import lax
from jax.experimental import pallas as pl
from jax.experimental.pallas import tpu as pltpu
from jax.sharding import PartitionSpec as P

LN_EPS = 1e-5
LOG2_E = 1.4426950408889634
UNROLL = 4


def layer_norm(hidden, gain, shift):
    hidden = hidden.astype(jnp.float32)
    centered = hidden - jnp.mean(hidden, axis=-1, keepdims=True)
    variance = jnp.mean(centered * centered, axis=-1, keepdims=True)
    return centered * lax.rsqrt(variance + LN_EPS) * gain + shift


def dot_rows(lhs, rhs):
    return lax.dot_general(lhs, rhs, (((1,), (0,)), ((), ())), preferred_element_type=jnp.float32)


def dot_cols(lhs, rhs):
    return lax.dot_general(lhs, rhs, (((1,), (1,)), ((), ())), preferred_element_type=jnp.float32)


def attention_kernel(head_dim, q_block, len_ref, q_ref, k_ref, v_ref, o_ref):
    seq, lanes = k_ref.shape
    real_keys = len_ref[pl.program_id(0)]
    scale = head_dim ** -0.5 * LOG2_E
    lane = lax.broadcasted_iota(jnp.int32, (1, lanes), 1)
    key_lane = lax.broadcasted_iota(jnp.int32, (seq, lanes), 1)
    key_ok = lax.broadcasted_iota(jnp.int32, (seq, lanes), 0) < real_keys
    pad_bias = jnp.where(key_ok, 0.0, -1e30)
    keys_f32 = k_ref[...].astype(jnp.float32)
    values = v_ref[...]
    heads = []
    for head in range(lanes // head_dim):
        spare = (head + 1) * head_dim % lanes
        own = (key_lane // head_dim == head) & key_ok
        heads.append((jnp.where(own, keys_f32, jnp.where(key_lane == spare, pad_bias, 0.0)).astype(jnp.bfloat16), spare))

    def block(i, carry):
        rows = pl.ds(pl.multiple_of(i * q_block, q_block), q_block)
        q_all = q_ref[rows, :].astype(jnp.float32)
        result = jnp.zeros((q_block, lanes), jnp.float32)
        for head, (keys, spare) in enumerate(heads):
            own = lane // head_dim == head
            query = jnp.where(own, q_all, jnp.where(lane == spare, 1.0, 0.0)).astype(jnp.bfloat16)
            scores = dot_cols(query, keys)
            top = jnp.max(scores, axis=-1, keepdims=True)
            weights = jnp.exp2((scores - top) * scale)
            total = jnp.sum(weights, axis=-1, keepdims=True)
            probs = (weights * (1.0 / total)).astype(jnp.bfloat16)
            result = jnp.where(own, dot_rows(probs, values), result)
        o_ref[rows, :] = result.astype(jnp.bfloat16)
        return carry

    lax.fori_loop(0, seq // q_block, block, 0, unroll=UNROLL)


def attend(query, keys, values, src_len, seq, head_dim):
    tokens, width = query.shape
    rows = tokens // seq
    lanes = 128
    spec = pl.BlockSpec((seq, lanes), lambda r, c, lens: (r, c))
    heads = width // head_dim
    return pl.pallas_call(
        functools.partial(attention_kernel, head_dim, 256),
        out_shape=jax.ShapeDtypeStruct((tokens, width), jnp.bfloat16),
        grid_spec=pltpu.PrefetchScalarGridSpec(num_scalar_prefetch=1, grid=(rows, width // lanes), in_specs=[spec, spec, spec], out_specs=spec),
        compiler_params=pltpu.CompilerParams(dimension_semantics=('arbitrary', 'arbitrary')),
        cost_estimate=pl.CostEstimate(flops=40 * rows * heads * seq * seq * head_dim, bytes_accessed=8 * tokens * width, transcendentals=rows * heads * seq * seq),
        name='attend',
    )(src_len, query, keys, values)


def attention_layer(residual, normed, src_len, seq, head_dim, w_q, b_q, w_k, w_v, b_v, w_o, b_o):
    query = (dot_cols(normed, w_q) + b_q).astype(jnp.bfloat16)
    keys = dot_cols(normed, w_k).astype(jnp.bfloat16)
    values = (dot_cols(normed, w_v) + b_v).astype(jnp.bfloat16)
    context = attend(query, keys, values, src_len, seq, head_dim)
    return (residual.astype(jnp.float32) + dot_rows(context, w_o) + b_o).astype(jnp.bfloat16)


def dense_ffn(residual, gain, shift, blocks, b_out):
    normed = layer_norm(residual, gain, shift).astype(jnp.bfloat16)
    projected = 0.0
    for w_in, b_in, w_out in blocks:
        inner = jax.nn.relu(dot_cols(normed, w_in) + b_in).astype(jnp.bfloat16)
        projected = projected + dot_rows(inner, w_out)
    return (residual.astype(jnp.float32) + projected + b_out).astype(jnp.bfloat16)


def route_slots(valid, first, second, num_experts, capacity):
    expert_ids = jnp.arange(num_experts, dtype=jnp.int32)
    hot_first = ((first[:, None] == expert_ids) & valid[:, None]).astype(jnp.int32)
    hot_second = ((second[:, None] == expert_ids) & valid[:, None]).astype(jnp.int32)
    rank_first = jnp.cumsum(hot_first, axis=0) - 1
    rank_second = jnp.cumsum(hot_second, axis=0) - 1 + jnp.sum(hot_first, axis=0)
    slot_first = jnp.sum(rank_first * hot_first, axis=1)
    slot_second = jnp.sum(rank_second * hot_second, axis=1)
    return slot_first, slot_second, valid & (slot_first < capacity), valid & (slot_second < capacity)


def solution(mesh):
    ep_size = mesh.shape['ep']
    tp_size = mesh.shape['tp']

    def gathered(shard):
        return lax.all_gather(shard, 'tp', axis=0, tiled=True)

    def local_fn(x, src_len, expert_idx, ln_gain, ln_bias, w_query, b_query, w_key, w_value, b_value, w_attn_out, b_attn_out, w_fc1, b_fc1, w_fc2, b_fc2, w_router, w_exp_in, b_exp_in, w_exp_out, b_exp_out):
        rows, seq_len, d_model = x.shape
        tokens = rows * seq_len
        num_experts = w_router.shape[1]
        capacity = 2 * (-(-tokens // num_experts))
        local_experts = w_exp_in.shape[0]
        layers, _, local_heads, head_dim = w_query.shape
        head_width = local_heads * head_dim
        part = capacity // tp_size
        own_rows = rows // tp_size
        me = lax.axis_index('tp')

        def whole(parts, height):
            return lax.all_gather(jnp.concatenate([w.reshape(-1, height, d_model) for w in parts], axis=0), 'tp', axis=1, tiled=True)

        def cols(w):
            return w.reshape(d_model, head_width).T

        biases = jnp.concatenate([b_query.reshape(-1), b_value.reshape(-1), b_fc1, b_exp_in.reshape(-1)])
        biases = lax.all_gather(biases, 'tp', axis=0)
        sizes = [layers * head_width, layers * head_width, b_fc1.shape[0], b_exp_in.size]
        offsets = [sum(sizes[:i]) for i in range(5)]
        b_q, b_v, b_in, b_expert = [biases[:, offsets[i]:offsets[i + 1]] for i in range(4)]
        b_q = b_q.reshape(tp_size, layers, head_width).transpose(1, 0, 2).reshape(layers, -1)
        b_v = b_v.reshape(tp_size, layers, head_width).transpose(1, 0, 2).reshape(layers, -1)
        b_expert = b_expert.reshape(tp_size, local_experts, -1).transpose(1, 0, 2).reshape(local_experts, -1)

        ep_me = lax.axis_index('ep')
        slab = w_fc1.shape[1] // ep_size
        slab_in = lax.dynamic_slice_in_dim(w_fc1, ep_me * slab, slab, 1).T
        slab_out = lax.dynamic_slice_in_dim(w_fc2, ep_me * slab, slab, 0)
        mine, choices = lax.optimization_barrier((whole([slab_in, slab_out], slab), expert_idx))
        cores = 2
        parts, owners = [mine], [ep_me]
        for step in range(cores, ep_size, cores):
            parts.append(lax.ppermute(mine, 'ep', [(e, (e + step) % ep_size) for e in range(ep_size)]))
            owners.append((ep_me + ep_size - step) % ep_size)
        owners = jnp.stack(owners)
        b_slabs = b_in.reshape(tp_size, ep_size, slab).transpose(1, 0, 2)

        def slab_bias(e):
            return jnp.sum(jnp.where((e[:, None] == jnp.arange(ep_size))[:, :, None, None], b_slabs[None], 0.0), axis=1).reshape(-1)

        sibling = ep_me + 1 - 2 * (ep_me % cores)
        other_owners = jnp.stack([(sibling + ep_size - step) % ep_size for step in range(0, ep_size, cores)])

        qkvo = whole([cols(w_query[0]), cols(w_key[0]), cols(w_value[0]), w_attn_out[0]], head_width)
        later = whole([cols(w_query[1]), cols(w_key[1]), cols(w_value[1]), w_attn_out[1]], head_width)
        second_weights = later[0], later[1], later[2], later[3]
        ff_part = w_exp_in.shape[2]

        def expert_weights(experts, after):
            parts, after = lax.optimization_barrier(([w for e in experts for w in (w_exp_in[e].T, w_exp_out[e])], after))
            both = whole(parts, ff_part)
            return [(both[2 * i], both[2 * i + 1]) for i in range(len(experts))], after


        first_weights = qkvo[0], qkvo[1], qkvo[2], qkvo[3]

        own_x = lax.dynamic_index_in_dim(x.reshape(own_rows, tp_size, seq_len, d_model), me, 1, keepdims=False).reshape(own_rows * seq_len, d_model)
        own_len = lax.dynamic_index_in_dim(src_len.reshape(own_rows, tp_size), me, 1, keepdims=False)

        def norm(v, i):
            return layer_norm(v, ln_gain[i], ln_bias[i]).astype(jnp.bfloat16)

        def attention(v, normed, lens, j, weights):
            w_q, w_k, w_v, w_o = weights
            return attention_layer(v, normed, lens, seq_len, head_dim, w_q, b_q[j], w_k, w_v, b_v[j], w_o, b_attn_out[j])

        expert_w, own_normed = expert_weights(list(range(local_experts // 2)), norm(own_x, 0))
        key_ok = jnp.arange(seq_len)[None, :] < src_len[:, None]
        valid = key_ok.reshape(tokens)
        first = choices[..., 0].reshape(tokens)
        second = choices[..., 1].reshape(tokens)
        slot_first, slot_second, keep_first, keep_second = route_slots(valid, first, second, num_experts, capacity)
        dump_slot = num_experts * capacity
        token_ids = jnp.arange(tokens, dtype=jnp.int32)
        table = jnp.zeros((dump_slot + 1,), jnp.int32)
        own_normed, slot_first, slot_second = lax.optimization_barrier((own_normed, slot_first, slot_second))
        own = attention(own_x, own_normed, own_len, 0, first_weights)
        parts, own = lax.optimization_barrier((parts, own))
        core_half = jnp.concatenate(parts, axis=1)
        other_half = lax.ppermute(core_half, 'ep', [(e, e ^ 1) for e in range(ep_size)])
        dense_blocks = [(core_half[0], slab_bias(owners), core_half[1]), (other_half[0], slab_bias(other_owners), other_half[1])]
        own = dense_ffn(own, ln_gain[1], ln_bias[1], dense_blocks, b_fc2)
        chunks = []
        for c in range(own_rows):
            row = own[c * seq_len:(c + 1) * seq_len]
            out = attention(row, norm(row, 2), own_len[c:c + 1], 1, second_weights)
            if c == 0:
                out, expert_w[0] = lax.optimization_barrier((out, expert_w[0]))
            if c == own_rows - 1:
                more, out = expert_weights(list(range(local_experts // 2, local_experts)), out)
                expert_w += more
            chunks.append(gathered(out))

        table = table.at[jnp.where(keep_first, first * capacity + slot_first, dump_slot)].set(token_ids)
        table = table.at[jnp.where(keep_second, second * capacity + slot_second, dump_slot)].set(token_ids)
        table = table[:dump_slot].reshape(ep_size, local_experts, tp_size, part)
        table = lax.dynamic_index_in_dim(table, me, 2, keepdims=False)

        hidden = jnp.concatenate(chunks, axis=0)
        normed_f32 = layer_norm(hidden, ln_gain[3], ln_bias[3])
        logits = jnp.dot(normed_f32, w_router, preferred_element_type=jnp.float32)
        expert_ids = jnp.arange(num_experts, dtype=jnp.int32)
        logit_first = jnp.sum(jnp.where(first[:, None] == expert_ids, logits, 0.0), axis=1)
        logit_second = jnp.sum(jnp.where(second[:, None] == expert_ids, logits, 0.0), axis=1)
        gate_first = jax.nn.sigmoid(logit_first - logit_second)
        gate_second = jax.nn.sigmoid(logit_second - logit_first)

        normed = normed_f32.astype(jnp.bfloat16)
        returned = []
        pair = local_experts // 2
        starts = range(0, local_experts, pair)
        dispatch = [normed[table[:, start:start + pair].reshape(-1)].reshape(ep_size, pair, part, d_model) for start in starts]
        for n, start in enumerate(starts):
            received = lax.all_to_all(dispatch[n], 'ep', 0, 0, tiled=True)
            if n == 0:
                received, *dispatch[1:] = lax.optimization_barrier((received, *dispatch[1:]))
            outs = []
            for e in range(start, start + pair):
                w_in, w_out = expert_w[e]
                inner = jax.nn.relu(dot_cols(received[:, e - start].reshape(-1, d_model), w_in) + b_expert[e]).astype(jnp.bfloat16)
                outs.append((dot_rows(inner, w_out) + b_exp_out[e]).astype(jnp.bfloat16).reshape(ep_size, part, d_model))
            back = lax.all_to_all(jnp.stack(outs, axis=1), 'ep', 0, 0, tiled=True)
            returned.append(gathered(back.reshape(-1, d_model)))
        flat = jnp.concatenate(returned, axis=0)

        def place(expert, slot):
            owner, e = expert // local_experts, expert % local_experts
            return (((e // pair * tp_size + slot // part) * ep_size + owner) * pair + e % pair) * part + slot % part

        out_first = flat[jnp.where(keep_first, place(first, slot_first), 0)].astype(jnp.float32)
        out_second = flat[jnp.where(keep_second, place(second, slot_second), 0)].astype(jnp.float32)
        combined = jnp.where(keep_first[:, None], gate_first[:, None] * out_first, 0.0) + jnp.where(keep_second[:, None], gate_second[:, None] * out_second, 0.0)
        return (hidden.astype(jnp.float32) + combined).astype(jnp.bfloat16).reshape(rows, seq_len, d_model)

    in_specs = (P(('dp', 'ep'), None, None), P(('dp', 'ep')), P(('dp', 'ep'), None, None), P(), P(), P(None, None, 'tp', None), P(None, 'tp', None), P(None, None, 'tp', None), P(None, None, 'tp', None), P(None, 'tp', None), P(None, 'tp', None, None), P(), P(None, 'tp'), P('tp'), P('tp', None), P(), P(), P('ep', None, 'tp'), P('ep', 'tp'), P('ep', 'tp', None), P('ep', None))
    return jax.shard_map(local_fn, mesh=mesh, in_specs=in_specs, out_specs=P(('dp', 'ep'), None, None), check_vma=False)
```
